128 devices in a mesh: data: 128 (over z, y, x, core).
Axes of the slice: x: 4, y: 4, z: 4, core: 2. Of those that a mesh axis runs over, the one named last changes fastest.
Arguments:
- z_one: bfloat16 [32768, 128], P('data')
- z_two: bfloat16 [32768, 128], P('data')
- z_small: bfloat16 [4, 32768, 128], P(None, 'data')
- protos: bfloat16 [3000, 128], replicated
- live_mask: int32 [32768], P('data')
Outputs:
- output 1: float32 [32768, 3000], P('data')
- output 2: float32 [32768, 3000], P('data')
- output 3: float32 [], replicated
- output 4: float32 [32768, 128], P('data')
- output 5: float32 [32768, 128], P('data')
- output 6: float32 [4, 32768, 128], P(None, 'data')
- output 7: float32 [3000, 128], replicated
All inputs are finite; a program needn't handle non-finite values.
Results may differ from the reference program's by a relative error of at most 0.001.
Values are sent between devices in bfloat16 or wider.
A program may use at most 1 GiB of HBM per device.

```python
import jax
import jax.numpy as jnp
from jax import lax

ROWS_DEV = 256
NUM_GROUPS = 128
NUM_PROTOS = 3000
EMBED_DIM = 128
SMALL_CROPS = 4
ITERS = 3
NUM_ROWS = ROWS_DEV * NUM_GROUPS
EPS = 0.05
TAU = 0.1


def unit_rows(matrix):
    return matrix / jnp.sqrt(jnp.sum(matrix * matrix, axis=-1, keepdims=True))


def draw_mask(mask_key):
    k_count, k_full, k_one, k_perm = jax.random.split(mask_key, 4)
    counts = jax.random.randint(k_count, (NUM_GROUPS,), 1, ROWS_DEV + 1)
    full_grp = jax.random.randint(k_full, (), 0, NUM_GROUPS)
    one_grp = (full_grp + jax.random.randint(k_one, (), 1, NUM_GROUPS)) % NUM_GROUPS
    groups = jnp.arange(NUM_GROUPS)
    counts = jnp.where(groups == full_grp, ROWS_DEV, counts)
    counts = jnp.where(groups == one_grp, 1, counts)
    perm_keys = jax.random.split(k_perm, NUM_GROUPS)
    rank_vals = jax.vmap(lambda perm_key: jax.random.permutation(perm_key, ROWS_DEV))(perm_keys)
    return (rank_vals < counts[:, None]).astype(jnp.int32).reshape(NUM_ROWS)


def draw_views(view_key, protos_f):
    k_pick, k_noise = jax.random.split(view_key)
    win_width = max(NUM_PROTOS // 2, 1)
    offsets = jax.random.randint(k_pick, (NUM_ROWS,), 0, win_width)
    win_start = (jnp.arange(NUM_ROWS) // ROWS_DEV) * NUM_PROTOS // NUM_GROUPS
    pick_ids = (win_start + offsets) % NUM_PROTOS
    centers = protos_f[pick_ids]
    noise_vals = jax.random.normal(k_noise, (2 + SMALL_CROPS, NUM_ROWS, EMBED_DIM), jnp.float32)
    mixed = 0.6 * centers[None] + 0.8 * noise_vals * EMBED_DIM ** -0.5
    return unit_rows(mixed).astype(jnp.bfloat16)


def setup_inputs(seed: int = 0) -> dict:
    root_key = jax.random.key(seed)
    k_proto, k_views, k_mask = jax.random.split(root_key, 3)
    protos_f = unit_rows(jax.random.normal(k_proto, (NUM_PROTOS, EMBED_DIM), jnp.float32))
    crops_all = draw_views(k_views, protos_f)
    return {"z_one": crops_all[0], "z_two": crops_all[1], "z_small": crops_all[2:], "protos": protos_f.astype(jnp.bfloat16), "live_mask": draw_mask(k_mask)}


def sinkhorn(scores, live_f, live_total):
    live_col = live_f[:, None]

    def sk_step(weights, unused):
        col_sum = jnp.sum(weights, axis=0)
        weights = weights / (NUM_PROTOS * col_sum)
        row_sum = jnp.sum(weights, axis=1, keepdims=True)
        row_safe = jnp.where(live_col > 0, row_sum, 1.0)
        weights = weights * (live_col / (live_total * row_safe))
        return weights, None

    weights = lax.scan(sk_step, live_col * jnp.exp(scores / EPS), None, length=ITERS)[0]
    return live_total * weights


def reference(z_one, z_two, z_small, protos, live_mask):
    live_f = live_mask.astype(jnp.float32)
    live_col = live_f[:, None]
    live_total = jnp.sum(live_f)
    pair_count = 2 + 2 * SMALL_CROPS
    grad_scale = 1.0 / (TAU * live_total * pair_count)
    scores_one = jnp.dot(z_one, protos.T, preferred_element_type=jnp.float32)
    scores_two = jnp.dot(z_two, protos.T, preferred_element_type=jnp.float32)
    q_one = sinkhorn(scores_one, live_f, live_total)
    q_two = sinkhorn(scores_two, live_f, live_total)
    q_sum = q_one + q_two
    logp_one = jax.nn.log_softmax(scores_one / TAU, axis=-1)
    logp_two = jax.nn.log_softmax(scores_two / TAU, axis=-1)
    grad_one = ((live_col * jnp.exp(logp_one) - q_two) * grad_scale).astype(jnp.bfloat16)
    grad_two = ((live_col * jnp.exp(logp_two) - q_one) * grad_scale).astype(jnp.bfloat16)

    def small_view(z_crop):
        scores = jnp.dot(z_crop, protos.T, preferred_element_type=jnp.float32)
        logp_crop = jax.nn.log_softmax(scores / TAU, axis=-1)
        grad_crop = ((2.0 * live_col * jnp.exp(logp_crop) - q_sum) * grad_scale).astype(jnp.bfloat16)
        return (jnp.sum(q_sum * logp_crop), jnp.dot(grad_crop, protos, preferred_element_type=jnp.float32), jnp.dot(grad_crop.T, z_crop, preferred_element_type=jnp.float32))

    small_cross, dz_small, small_dc = lax.map(small_view, z_small)
    cross_sum = jnp.sum(q_two * logp_one) + jnp.sum(q_one * logp_two) + jnp.sum(small_cross)
    loss_total = -cross_sum / (live_total * pair_count)
    dz_one = jnp.dot(grad_one, protos, preferred_element_type=jnp.float32)
    dz_two = jnp.dot(grad_two, protos, preferred_element_type=jnp.float32)
    d_protos = jnp.dot(grad_one.T, z_one, preferred_element_type=jnp.float32) + jnp.dot(grad_two.T, z_two, preferred_element_type=jnp.float32) + jnp.sum(small_dc, axis=0)
    return (q_one, q_two, loss_total, dz_one, dz_two, dz_small, d_protos)
```

```python
import functools
import itertools

import jax
import jax.numpy as jnp
from jax import lax
from jax.experimental import pallas as pl
from jax.experimental.pallas import tpu as pltpu
from jax.sharding import PartitionSpec as P

EPS = 0.05
TAU = 0.1
ITERS = 3
LOG2E = 1.4426950408889634
ROWS = 256
NUM_K = 3000
PAD_K = 3072
TILES = PAD_K // 128
FULL = 11
CHUNK = 256
TAIL = NUM_K - FULL * CHUNK
VIEWS = 6

MESH = pl.DeviceIdType.MESH
STRIDE = {"x": 2, "y": 8, "z": 32}


def group_of(me, axes):
    pos = {a: lax.rem(lax.div(me, STRIDE[a]), 4) for a in axes}
    base = me
    own = 0
    for a in axes:
        base = base - pos[a] * STRIDE[a]
        own = own * 4 + pos[a]
    others = []
    for offs in itertools.product(range(4), repeat=len(axes)):
        if any(offs):
            slot, dev = 0, base
            for a, o in zip(axes, offs):
                q = lax.rem(pos[a] + o, 4)
                slot = slot * 4 + q
                dev = dev + q * STRIDE[a]
            others.append((slot, dev))
    return own, others


def enter(devs):
    bar = pltpu.get_barrier_semaphore()
    for d in devs:
        pl.semaphore_signal(bar, inc=1, device_id=(d,), device_id_type=MESH)
    return lambda: pl.semaphore_wait(bar, len(devs))


def codes_kernel(z_ref, c_ref, m_ref, b_ref, rows_ref, live_ref,
                 zx, mcol, e, colsum, b8, dcol, drecv, slots_a, slots_b,
                 zsend, zrecv, asend, arecv, bsend, brecv, fsend, frecv):
    me = lax.axis_index("data")
    core = lax.rem(me, 2)
    mate = me + 1 - 2 * core
    own_a, others_a = group_of(me, "xy")
    own_b, others_b = group_of(me, "z")
    entered = enter([mate] + [d for _, d in others_a] + [d for _, d in others_b])

    mrow = jnp.broadcast_to(m_ref[...].astype(jnp.float32), (128, ROWS))
    mcol[0] = jnp.concatenate([mrow[:, :128].T, mrow[:, 128:].T], axis=0)

    def build(half, z_half):
        mk = mcol[half][:, :1]

        def piece(scores):
            return jnp.exp2(scores * (LOG2E / EPS)) * mk

        def step(i, carry):
            at = pl.multiple_of(i * CHUNK, CHUNK)
            s = lax.dot_general(z_half, c_ref[pl.ds(at, CHUNK), :], (((1,), (1,)), ((), ())),
                                preferred_element_type=jnp.float32)
            v = piece(s)
            e[pl.ds(half * ROWS, ROWS), pl.ds(at, CHUNK)] = v
            part = jnp.sum(v, axis=0, keepdims=True)
            if half:
                colsum[:, pl.ds(at, CHUNK)] += part
            else:
                colsum[:, pl.ds(at, CHUNK)] = part
            return carry

        lax.fori_loop(0, FULL, step, 0)
        s = lax.dot_general(z_half, c_ref[FULL * CHUNK:NUM_K, :], (((1,), (1,)), ((), ())),
                            preferred_element_type=jnp.float32)
        v = piece(s)
        e[half * ROWS:(half + 1) * ROWS, FULL * CHUNK + 128:] = jnp.zeros((ROWS, 128), jnp.float32)
        e[half * ROWS:(half + 1) * ROWS, FULL * CHUNK:NUM_K] = v
        part = jnp.sum(v, axis=0, keepdims=True)
        if half:
            colsum[:, FULL * CHUNK:NUM_K] += part
        else:
            colsum[:, FULL * CHUNK + 128:] = jnp.zeros((1, 128), jnp.float32)
            colsum[:, FULL * CHUNK:NUM_K] = part

    entered()
    give_z = pltpu.make_async_remote_copy(z_ref.at[1 - core], zx, zsend.at[0], zrecv.at[0],
                                          device_id=(mate,), device_id_type=MESH)
    give_m = pltpu.make_async_remote_copy(mcol.at[0], mcol.at[1], zsend.at[1], zrecv.at[1],
                                          device_id=(mate,), device_id_type=MESH)
    give_z.start()
    give_m.start()
    build(0, z_ref[core])
    give_z.wait()
    give_m.wait()
    build(1, zx[...])

    lane = lax.broadcasted_iota(jnp.int32, (1, 128), 1)
    flat = lax.broadcasted_iota(jnp.int32, (TILES, 128), 0) * 128 + lax.broadcasted_iota(jnp.int32, (TILES, 128), 1)
    count = jnp.sum(mcol[0] + mcol[1], axis=0, keepdims=True)

    def lse_of(view):
        z_view = z_ref[view]

        def step(i, acc):
            at = pl.multiple_of(i * CHUNK, CHUNK)
            s = lax.dot_general(z_view, c_ref[pl.ds(at, CHUNK), :], (((1,), (1,)), ((), ())),
                                preferred_element_type=jnp.float32)
            t = jnp.exp2(s * (LOG2E / TAU))
            return acc + t[:, :128] + t[:, 128:]

        acc = lax.fori_loop(0, FULL, step, jnp.zeros((ROWS, 128), jnp.float32))
        s = lax.dot_general(z_view, c_ref[FULL * CHUNK:NUM_K, :], (((1,), (1,)), ((), ())),
                            preferred_element_type=jnp.float32)
        t = jnp.exp2(s * (LOG2E / TAU))
        total = jnp.sum(acc, axis=1, keepdims=True) + jnp.sum(t, axis=1, keepdims=True)
        rows_ref[:, 2 + view:3 + view] = jnp.log(total)

    def exchange(slots, send, recv, it, own, others, work):
        copies = []
        for k, (_, dev) in enumerate(others):
            copies.append(pltpu.make_async_remote_copy(
                slots.at[it, own], slots.at[it, own], send.at[it, k], recv.at[it, own],
                device_id=(dev,), device_id_type=MESH))
            copies[-1].start()
        work()
        for slot, dev in others:
            pltpu.make_async_remote_copy(
                slots.at[it, slot], slots.at[it, slot], send.at[it, 0], recv.at[it, slot],
                device_id=(dev,), device_id_type=MESH).wait_recv()
        total = slots[it, 0]
        for q in range(1, len(others) + 1):
            total = total + slots[it, q]
        return total, copies

    pending = []
    for it in range(ITERS):
        for t in range(TILES):
            row = colsum[:, t * 128:(t + 1) * 128]
            if it == 0 and t == TILES - 1:
                row = jnp.where(lane == NUM_K % 128, count, row)
            slots_a[it, own_a, t:t + 1, :] = row
        total, copies = exchange(slots_a, asend, arecv, it, own_a, others_a, functools.partial(lse_of, 2 * it))
        pending += copies
        slots_b[it, own_b] = total
        total, copies = exchange(slots_b, bsend, brecv, it, own_b, others_b, functools.partial(lse_of, 2 * it + 1))
        pending += copies
        if it == 0:
            live_ref[...] = jnp.broadcast_to(total[TILES - 1:TILES, NUM_K % 128:NUM_K % 128 + 1], (8, 128))
        inside = flat < NUM_K
        bmat = jnp.where(inside, 1.0 / (NUM_K * jnp.where(inside, total, 1.0)), 0.0)
        if it == ITERS - 1:
            b_ref[core] = bmat
            give_b = pltpu.make_async_remote_copy(b_ref.at[core], b_ref.at[core], fsend.at[0], frecv.at[0],
                                                  device_id=(mate,), device_id_type=MESH)
            give_b.start()
        for t in range(TILES):
            b8[:, t * 128:(t + 1) * 128] = jnp.broadcast_to(bmat[t:t + 1, :], (8, 128))
        if it < ITERS - 1:
            colsum[...] = jnp.zeros_like(colsum)

        def block(i, carry):
            r0 = pl.multiple_of(i * 128, 128)
            acc = jnp.zeros((128, 128), jnp.float32)
            for t in range(TILES):
                acc += (e[pl.ds(r0, 128), t * 128:(t + 1) * 128].reshape(16, 8, 128)
                        * b8[:, t * 128:(t + 1) * 128][None]).reshape(128, 128)
            d = jnp.sum(acc, axis=1, keepdims=True)
            a = jnp.where(d > 0, 1.0 / jnp.where(d > 0, d, 1.0), 0.0)
            if it == ITERS - 1:
                dcol[pl.ds(r0, 128), :] = jnp.broadcast_to(a, (128, 128))
            else:
                ab = jnp.broadcast_to(a, (128, 128))
                for t in range(TILES):
                    colsum[:, t * 128:(t + 1) * 128] += jnp.sum(
                        e[pl.ds(r0, 128), t * 128:(t + 1) * 128] * ab, axis=0, keepdims=True)
            return carry

        lax.fori_loop(0, 2 * ROWS // 128, block, 0)

    give_a = pltpu.make_async_remote_copy(dcol.at[pl.ds(ROWS, ROWS)], drecv, fsend.at[1], frecv.at[1],
                                          device_id=(mate,), device_id_type=MESH)
    give_a.start()
    for c in pending:
        c.wait_send()
    give_b.wait_send()
    pltpu.make_async_remote_copy(b_ref.at[1 - core], b_ref.at[1 - core], fsend.at[0], frecv.at[0],
                                 device_id=(mate,), device_id_type=MESH).wait_recv()
    give_a.wait()
    first = core == 0
    own_r = dcol[:ROWS, :1]
    mate_r = drecv[:, :1]
    rows_ref[:, 0:1] = jnp.where(first, own_r, mate_r)
    rows_ref[:, 1:2] = jnp.where(first, mate_r, own_r)


def run_codes(z_all, protos, mask_row):
    vmem = pl.BlockSpec(memory_space=pltpu.VMEM)
    dma = pltpu.SemaphoreType.DMA
    return pl.pallas_call(
        codes_kernel,
        out_shape=(jax.ShapeDtypeStruct((2, TILES, 128), jnp.float32),
                   jax.ShapeDtypeStruct((ROWS, 128), jnp.float32),
                   jax.ShapeDtypeStruct((8, 128), jnp.float32)),
        in_specs=[vmem] * 3,
        out_specs=(vmem,) * 3,
        scratch_shapes=[
            pltpu.VMEM((ROWS, 128), jnp.bfloat16),
            pltpu.VMEM((2, ROWS, 128), jnp.float32),
            pltpu.VMEM((2 * ROWS, PAD_K), jnp.float32),
            pltpu.VMEM((1, PAD_K), jnp.float32),
            pltpu.VMEM((8, PAD_K), jnp.float32),
            pltpu.VMEM((2 * ROWS, 128), jnp.float32),
            pltpu.VMEM((ROWS, 128), jnp.float32),
            pltpu.VMEM((ITERS, 16, TILES, 128), jnp.float32),
            pltpu.VMEM((ITERS, 4, TILES, 128), jnp.float32),
            dma((2,)), dma((2,)),
            dma((ITERS, 15)), dma((ITERS, 16)),
            dma((ITERS, 3)), dma((ITERS, 4)),
            dma((2,)), dma((2,)),
        ],
        name="codes",
        compiler_params=pltpu.CompilerParams(collective_id=0, has_side_effects=True),
    )(z_all, protos, mask_row)


def local_step(z_one, z_two, z_small, protos, live_mask):
    live_col = live_mask.astype(jnp.float32)[:, None]
    z_all = jnp.concatenate([z_one[None], z_two[None], z_small], axis=0)
    bmat, rows, live = run_codes(z_all, protos, live_mask[None, :])
    live_total = live[0, 0]
    pair_count = 2 + 2 * z_small.shape[0]
    grad_scale = 1.0 / (TAU * live_total * pair_count)
    b = bmat.reshape(2, 1, PAD_K)[:, :, :NUM_K]
    scores = jnp.einsum("vnd,kd->vnk", z_all, protos, preferred_element_type=jnp.float32)
    q = jnp.exp(scores[:2] / EPS) * b * rows[:, :2].T[:, :, None]
    logp = scores / TAU - rows[:, 2:8].T[:, :, None]
    q_one, q_two = q[0], q[1]
    q_sum = q_one + q_two
    cross_sum = jnp.sum(q_two * logp[0]) + jnp.sum(q_one * logp[1]) + jnp.sum(q_sum[None] * logp[2:])
    grad_one = ((live_col * jnp.exp(logp[0]) - q_two) * grad_scale).astype(jnp.bfloat16)
    grad_two = ((live_col * jnp.exp(logp[1]) - q_one) * grad_scale).astype(jnp.bfloat16)
    grad_small = ((2.0 * live_col[None] * jnp.exp(logp[2:]) - q_sum[None]) * grad_scale).astype(jnp.bfloat16)
    grads = jnp.concatenate([grad_one[None], grad_two[None], grad_small], axis=0)
    dz = jnp.einsum("jnk,kd->jnd", grads, protos, preferred_element_type=jnp.float32)
    dc_part = jnp.einsum("jnk,jnd->kd", grads, z_all, preferred_element_type=jnp.float32)
    d_protos = lax.psum(dc_part, "data")
    loss_total = -lax.psum(cross_sum, "data") / (live_total * pair_count)
    return q_one, q_two, loss_total, dz[0], dz[1], dz[2:], d_protos


def solution(mesh):
    row_spec = P("data", None)
    crop_spec = P(None, "data", None)
    return jax.shard_map(local_step, mesh=mesh,
                         in_specs=(row_spec, row_spec, crop_spec, P(None, None), P("data")),
                         out_specs=(row_spec, row_spec, P(), row_spec, row_spec, crop_spec, P(None, None)),
                         check_vma=False)
```

```python
import functools
import itertools

import jax
import jax.numpy as jnp
from jax import lax
from jax.experimental import pallas as pl
from jax.experimental.pallas import tpu as pltpu
from jax.sharding import PartitionSpec as P

EPS = 0.05
TAU = 0.1
ITERS = 3
LOG2E = 1.4426950408889634
ROWS = 256
NUM_K = 3000
PAD_K = 3072
TILES = PAD_K // 128
FULL = 11
CHUNK = 256
TAIL = NUM_K - FULL * CHUNK
VIEWS = 6

MESH = pl.DeviceIdType.MESH
STRIDE = {"x": 2, "y": 8, "z": 32}


def group_of(me, axes):
    pos = {a: lax.rem(lax.div(me, STRIDE[a]), 4) for a in axes}
    base = me
    own = 0
    for a in axes:
        base = base - pos[a] * STRIDE[a]
        own = own * 4 + pos[a]
    others = []
    for offs in itertools.product(range(4), repeat=len(axes)):
        if any(offs):
            slot, dev = 0, base
            for a, o in zip(axes, offs):
                q = lax.rem(pos[a] + o, 4)
                slot = slot * 4 + q
                dev = dev + q * STRIDE[a]
            others.append((slot, dev))
    return own, others


def enter(devs):
    bar = pltpu.get_barrier_semaphore()
    for d in devs:
        pl.semaphore_signal(bar, inc=1, device_id=(d,), device_id_type=MESH)
    return lambda: pl.semaphore_wait(bar, len(devs))


def codes_kernel(z1_ref, z2_ref, zs_ref, c_ref, m_ref, b_ref, rows_ref, live_ref,
                 z_ref, zx, mcol, e, colsum, dcol, drecv, slots_a, slots_b,
                 zsend, zrecv, asend, arecv, bsend, brecv, fsend, frecv):
    me = lax.axis_index("data")
    core = lax.rem(me, 2)
    mate = me + 1 - 2 * core
    own_a, others_a = group_of(me, "xy")
    own_b, others_b = group_of(me, "z")
    entered = enter([mate] + [d for _, d in others_a] + [d for _, d in others_b])

    z_ref[0] = z1_ref[...]
    z_ref[1] = z2_ref[...]
    mrow = jnp.broadcast_to(m_ref[...].astype(jnp.float32), (128, ROWS))
    mcol[0] = jnp.concatenate([mrow[:, :128].T, mrow[:, 128:].T], axis=0)

    def build(half, z_half):
        mk = mcol[half][:, :1]

        def piece(scores):
            return jnp.exp2(scores * (LOG2E / EPS)) * mk

        def step(i, carry):
            at = pl.multiple_of(i * CHUNK, CHUNK)
            s = lax.dot_general(z_half, c_ref[pl.ds(at, CHUNK), :], (((1,), (1,)), ((), ())),
                                preferred_element_type=jnp.float32)
            v = piece(s)
            e[pl.ds(half * ROWS, ROWS), pl.ds(at, CHUNK)] = v
            part = jnp.sum(v, axis=0, keepdims=True)
            if half:
                colsum[:, pl.ds(at, CHUNK)] += part
            else:
                colsum[:, pl.ds(at, CHUNK)] = part
            return carry

        lax.fori_loop(0, FULL, step, 0)
        s = lax.dot_general(z_half, c_ref[FULL * CHUNK:NUM_K, :], (((1,), (1,)), ((), ())),
                            preferred_element_type=jnp.float32)
        v = piece(s)
        e[half * ROWS:(half + 1) * ROWS, FULL * CHUNK + 128:] = jnp.zeros((ROWS, 128), jnp.float32)
        e[half * ROWS:(half + 1) * ROWS, FULL * CHUNK:NUM_K] = v
        part = jnp.sum(v, axis=0, keepdims=True)
        if half:
            colsum[:, FULL * CHUNK:NUM_K] += part
        else:
            colsum[:, FULL * CHUNK + 128:] = jnp.zeros((1, 128), jnp.float32)
            colsum[:, FULL * CHUNK:NUM_K] = part

    entered()
    give_z = pltpu.make_async_remote_copy(z_ref.at[1 - core], zx, zsend.at[0], zrecv.at[0],
                                          device_id=(mate,), device_id_type=MESH)
    give_m = pltpu.make_async_remote_copy(mcol.at[0], mcol.at[1], zsend.at[1], zrecv.at[1],
                                          device_id=(mate,), device_id_type=MESH)
    give_z.start()
    give_m.start()
    build(0, z_ref[core])
    give_z.wait()
    give_m.wait()
    build(1, zx[...])

    lane = lax.broadcasted_iota(jnp.int32, (1, 128), 1)
    flat = lax.broadcasted_iota(jnp.int32, (TILES, 128), 0) * 128 + lax.broadcasted_iota(jnp.int32, (TILES, 128), 1)
    count = jnp.sum(mcol[0] + mcol[1], axis=0, keepdims=True)

    def lse_of(view):
        z_view = z_ref[view] if view < 2 else zs_ref[view - 2]

        def step(i, acc):
            at = pl.multiple_of(i * CHUNK, CHUNK)
            s = lax.dot_general(z_view, c_ref[pl.ds(at, CHUNK), :], (((1,), (1,)), ((), ())),
                                preferred_element_type=jnp.float32)
            t = jnp.exp2(s * (LOG2E / TAU))
            return acc + t[:, :128] + t[:, 128:]

        acc = lax.fori_loop(0, FULL, step, jnp.zeros((ROWS, 128), jnp.float32))
        s = lax.dot_general(z_view, c_ref[FULL * CHUNK:NUM_K, :], (((1,), (1,)), ((), ())),
                            preferred_element_type=jnp.float32)
        t = jnp.exp2(s * (LOG2E / TAU))
        total = jnp.sum(acc, axis=1, keepdims=True) + jnp.sum(t, axis=1, keepdims=True)
        live = mcol[0][:, :1]
        rows_ref[:, 2 + view:3 + view] = live / total
        lse = jnp.log(total) * (live if view < 2 else 2.0 * live)
        rows_ref[:, 8:9] = lse if view == 0 else rows_ref[:, 8:9] + lse

    def exchange(slots, send, recv, it, own, others, work):
        copies = []
        for k, (_, dev) in enumerate(others):
            copies.append(pltpu.make_async_remote_copy(
                slots.at[it, own], slots.at[it, own], send.at[it, k], recv.at[it, own],
                device_id=(dev,), device_id_type=MESH))
            copies[-1].start()
        work()
        for slot, dev in others:
            pltpu.make_async_remote_copy(
                slots.at[it, slot], slots.at[it, slot], send.at[it, 0], recv.at[it, slot],
                device_id=(dev,), device_id_type=MESH).wait_recv()
        total = slots[it, 0]
        for q in range(1, len(others) + 1):
            total = total + slots[it, q]
        return total, copies

    pending = []
    for it in range(ITERS):
        for t in range(TILES):
            row = colsum[:, t * 128:(t + 1) * 128]
            if it == 0 and t == TILES - 1:
                row = jnp.where(lane == NUM_K % 128, count, row)
            slots_a[it, own_a, t:t + 1, :] = row
        total, copies = exchange(slots_a, asend, arecv, it, own_a, others_a, functools.partial(lse_of, 2 * it))
        pending += copies
        slots_b[it, own_b] = total
        total, copies = exchange(slots_b, bsend, brecv, it, own_b, others_b, functools.partial(lse_of, 2 * it + 1))
        pending += copies
        if it == 0:
            live_ref[...] = jnp.broadcast_to(total[TILES - 1:TILES, NUM_K % 128:NUM_K % 128 + 1], (8, 128))
        inside = flat < NUM_K
        bmat = jnp.where(inside, 1.0 / (NUM_K * jnp.where(inside, total, 1.0)), 0.0)
        for t in range(TILES):
            b_ref[core, :, t * 128:(t + 1) * 128] = jnp.broadcast_to(bmat[t:t + 1, :], (8, 128))
        if it == ITERS - 1:
            give_b = pltpu.make_async_remote_copy(b_ref.at[core], b_ref.at[core], fsend.at[0], frecv.at[0],
                                                  device_id=(mate,), device_id_type=MESH)
            give_b.start()
        if it < ITERS - 1:
            colsum[...] = jnp.zeros_like(colsum)

        def block(i, carry):
            r0 = pl.multiple_of(i * 128, 128)
            acc = jnp.zeros((128, 128), jnp.float32)
            for t in range(TILES):
                acc += (e[pl.ds(r0, 128), t * 128:(t + 1) * 128].reshape(16, 8, 128)
                        * b_ref[core, :, t * 128:(t + 1) * 128][None]).reshape(128, 128)
            d = jnp.sum(acc, axis=1, keepdims=True)
            a = jnp.where(d > 0, 1.0 / jnp.where(d > 0, d, 1.0), 0.0)
            if it == ITERS - 1:
                dcol[pl.ds(r0, 128), :] = jnp.broadcast_to(a, (128, 128))
            else:
                ab = jnp.broadcast_to(a, (128, 128))
                for t in range(TILES):
                    colsum[:, t * 128:(t + 1) * 128] += jnp.sum(
                        e[pl.ds(r0, 128), t * 128:(t + 1) * 128] * ab, axis=0, keepdims=True)
            return carry

        lax.fori_loop(0, 2 * ROWS // 128, block, 0)

    give_a = pltpu.make_async_remote_copy(dcol.at[pl.ds(ROWS, ROWS)], drecv, fsend.at[1], frecv.at[1],
                                          device_id=(mate,), device_id_type=MESH)
    give_a.start()
    for c in pending:
        c.wait_send()
    give_b.wait_send()
    pltpu.make_async_remote_copy(b_ref.at[1 - core], b_ref.at[1 - core], fsend.at[0], frecv.at[0],
                                 device_id=(mate,), device_id_type=MESH).wait_recv()
    give_a.wait()
    first = core == 0
    own_r = dcol[:ROWS, :1]
    mate_r = drecv[:, :1]
    rows_ref[:, 0:1] = jnp.where(first, own_r, mate_r)
    rows_ref[:, 1:2] = jnp.where(first, mate_r, own_r)


def run_codes(z_one, z_two, z_small, protos, mask_row):
    vmem = pl.BlockSpec(memory_space=pltpu.VMEM)
    dma = pltpu.SemaphoreType.DMA
    return pl.pallas_call(
        codes_kernel,
        out_shape=(jax.ShapeDtypeStruct((2, 8, PAD_K), jnp.float32),
                   jax.ShapeDtypeStruct((ROWS, 128), jnp.float32),
                   jax.ShapeDtypeStruct((8, 128), jnp.float32)),
        in_specs=[vmem] * 5,
        out_specs=(vmem,) * 3,
        scratch_shapes=[
            pltpu.VMEM((2, ROWS, 128), jnp.bfloat16),
            pltpu.VMEM((ROWS, 128), jnp.bfloat16),
            pltpu.VMEM((2, ROWS, 128), jnp.float32),
            pltpu.VMEM((2 * ROWS, PAD_K), jnp.float32),
            pltpu.VMEM((1, PAD_K), jnp.float32),
            pltpu.VMEM((2 * ROWS, 128), jnp.float32),
            pltpu.VMEM((ROWS, 128), jnp.float32),
            pltpu.VMEM((ITERS, 16, TILES, 128), jnp.float32),
            pltpu.VMEM((ITERS, 4, TILES, 128), jnp.float32),
            dma((2,)), dma((2,)),
            dma((ITERS, 15)), dma((ITERS, 16)),
            dma((ITERS, 3)), dma((ITERS, 4)),
            dma((2,)), dma((2,)),
        ],
        name="codes",
        compiler_params=pltpu.CompilerParams(collective_id=0, has_side_effects=True),
    )(z_one, z_two, z_small, protos, mask_row)


KC = 512
STEPS = PAD_K // KC
RB = 16


def grads_kernel(z1_ref, z2_ref, zs_ref, c_ref, b_ref, rows_ref, live_ref,
                 q1_ref, q2_ref, dz1_ref, dz2_ref, dzs_ref, dc_ref,
                 zall, cm, s_all, g_all, dz_acc, loss_acc):
    i = pl.program_id(0)

    @pl.when(i == 0)
    def _():
        zall[0:ROWS] = z1_ref[...]
        zall[ROWS:2 * ROWS] = z2_ref[...]
        for j in range(4):
            zall[(2 + j) * ROWS:(3 + j) * ROWS] = zs_ref[j]
        dz_acc[...] = jnp.zeros_like(dz_acc)
        loss_acc[...] = jnp.zeros_like(loss_acc)

    row_id = lax.broadcasted_iota(jnp.int32, (KC, 128), 0) + i * KC
    cm[...] = jnp.where(row_id < NUM_K, c_ref[...].astype(jnp.float32), 0.0).astype(jnp.bfloat16)
    s_all[...] = lax.dot_general(zall[...], cm[...], (((1,), (1,)), ((), ())), preferred_element_type=jnp.float32)
    g = 1.0 / (TAU * 10.0 * live_ref[0:1, 0:1])

    def block(n, acc):
        at = pl.multiple_of(n * RB, RB)
        rows = rows_ref[pl.ds(at, RB), :]
        b = [jnp.broadcast_to(b_ref[v][None], (RB // 8, 8, KC)).reshape(RB, KC) for v in range(2)]
        s = [s_all[pl.ds(pl.multiple_of(v * ROWS + at, RB), RB), :] for v in range(VIEWS)]
        t = [jnp.exp2(x * (LOG2E / TAU)) for x in s]
        q1 = (t[0] * rows[:, 0:1]) * (t[0] * b[0])
        q2 = (t[1] * rows[:, 1:2]) * (t[1] * b[1])
        q1_ref[pl.ds(at, RB), :] = q1
        q2_ref[pl.ds(at, RB), :] = q2
        small = (s[2] + s[3]) + (s[4] + s[5])
        term = q2 * (s[0] + small) + q1 * (s[1] + small)
        gq1 = q1 * g
        gq2 = q2 * g
        gqs = gq1 + gq2
        for v in range(VIEWS):
            w = rows[:, 2 + v:3 + v] * (g if v < 2 else 2.0 * g)
            sub = (gq2, gq1)[v] if v < 2 else gqs
            g_all[pl.ds(pl.multiple_of(v * ROWS + at, RB), RB), :] = (t[v] * w - sub).astype(jnp.bfloat16)
        for r in range(RB // 8):
            for k in range(KC // 128):
                acc = acc + term[r * 8:(r + 1) * 8, k * 128:(k + 1) * 128]
        return acc

    loss_acc[...] = lax.fori_loop(0, ROWS // RB, block, loss_acc[...])
    dz_acc[...] += lax.dot_general(g_all[...], cm[...], (((1,), (0,)), ((), ())), preferred_element_type=jnp.float32)
    dc_ref[...] = lax.dot_general(g_all[...], zall[...], (((0,), (0,)), ((), ())), preferred_element_type=jnp.float32)

    @pl.when(i == STEPS - 1)
    def _():
        dz1_ref[...] = dz_acc[0:ROWS]
        dz2_ref[...] = dz_acc[ROWS:2 * ROWS]
        for j in range(4):
            dzs_ref[j] = dz_acc[(2 + j) * ROWS:(3 + j) * ROWS]
        lse = jnp.sum(rows_ref[:, 8:9])
        lane0 = ((lax.broadcasted_iota(jnp.int32, (8, 128), 0) == 0)
                 & (lax.broadcasted_iota(jnp.int32, (8, 128), 1) == 0))
        tail = NUM_K - (STEPS - 1) * KC
        dc_ref[tail:tail + 8, :] = loss_acc[...] * (1.0 / TAU) - jnp.where(lane0, lse, 0.0)


def run_grads(z_one, z_two, z_small, protos, b, rows, live):
    def whole(*shape):
        return pl.BlockSpec(shape, lambda i: (0,) * len(shape))

    f32 = jnp.float32
    return pl.pallas_call(
        grads_kernel,
        grid=(STEPS,),
        out_shape=(jax.ShapeDtypeStruct((ROWS, NUM_K), f32), jax.ShapeDtypeStruct((ROWS, NUM_K), f32),
                   jax.ShapeDtypeStruct((ROWS, 128), f32), jax.ShapeDtypeStruct((ROWS, 128), f32),
                   jax.ShapeDtypeStruct((4, ROWS, 128), f32), jax.ShapeDtypeStruct((PAD_K, 128), f32)),
        in_specs=[whole(ROWS, 128), whole(ROWS, 128), whole(4, ROWS, 128),
                  pl.BlockSpec((KC, 128), lambda i: (i, 0)),
                  pl.BlockSpec((2, 8, KC), lambda i: (0, 0, i)),
                  whole(ROWS, 128), whole(8, 128)],
        out_specs=(pl.BlockSpec((ROWS, KC), lambda i: (0, i)), pl.BlockSpec((ROWS, KC), lambda i: (0, i)),
                   whole(ROWS, 128), whole(ROWS, 128), whole(4, ROWS, 128),
                   pl.BlockSpec((KC, 128), lambda i: (i, 0))),
        scratch_shapes=[
            pltpu.VMEM((VIEWS * ROWS, 128), jnp.bfloat16),
            pltpu.VMEM((KC, 128), jnp.bfloat16),
            pltpu.VMEM((VIEWS * ROWS, KC), f32),
            pltpu.VMEM((VIEWS * ROWS, KC), jnp.bfloat16),
            pltpu.VMEM((VIEWS * ROWS, 128), f32),
            pltpu.VMEM((8, 128), f32),
        ],
        name="grads",
        compiler_params=pltpu.CompilerParams(dimension_semantics=("arbitrary",)),
    )(z_one, z_two, z_small, protos, b, rows, live)


HALF = PAD_K // 2
THIRD = HALF // 3
ORDERS = (("x", "yz"), ("y", "xz"), ("z", "xy"))


def total_kernel(part_ref, out_ref, r0, acc, r1, mid, r2,
                 s0, v0, s1, v1, s2, v2, s3, v3, s4, v4, s5, v5):
    me = lax.axis_index("data")
    core = lax.rem(me, 2)
    mate = me + 1 - 2 * core
    lines = [group_of(me, a) for a, _ in ORDERS]
    planes = [group_of(me, p) for _, p in ORDERS]
    devs = [mate]
    for _, others in lines:
        devs += [d for _, d in others]
    for n, (_, others) in enumerate(planes):
        axes = ORDERS[n][1]
        devs += [d for (_, d), offs in zip(others, [o for o in itertools.product(range(4), repeat=2) if any(o)]) if all(offs)]
    enter(devs)()
    mine = pl.multiple_of(core * HALF, HALF)
    theirs = pl.multiple_of((1 - core) * HALF, HALF)
    pending = []

    def send(src, dst, ssem, rsem, dev):
        c = pltpu.make_async_remote_copy(src, dst, ssem, rsem, device_id=(dev,), device_id_type=MESH)
        c.start()
        pending.append(c)

    def arrived(dst, ssem, rsem, dev):
        pltpu.make_async_remote_copy(dst, dst, ssem, rsem, device_id=(dev,), device_id_type=MESH).wait_recv()

    for j in range(3):
        send(part_ref.at[pl.ds(theirs + j * THIRD, THIRD)], r0.at[j], s0.at[j], v0.at[j], mate)
    for j in range(3):
        arrived(r0.at[j], s0.at[j], v0.at[j], mate)
        acc[j] = part_ref[pl.ds(mine + j * THIRD, THIRD), :] + r0[j]
        own, others = lines[j]
        for k, (slot, dev) in enumerate(others):
            send(acc.at[j, pl.ds(pl.multiple_of(slot * 128, 128), 128)], r1.at[j, own], s1.at[j, k], v1.at[j, own], dev)
        r1[j, own] = acc[j, pl.ds(pl.multiple_of(own * 128, 128), 128), :]
    for j in range(3):
        own, others = lines[j]
        for k, (slot, dev) in enumerate(others):
            arrived(r1.at[j, slot], s1.at[j, k], v1.at[j, slot], dev)
        mid[j] = (r1[j, 0] + r1[j, 1]) + (r1[j, 2] + r1[j, 3])
        own, others = planes[j]
        for k, (slot, dev) in enumerate(others):
            send(mid.at[j, pl.ds(pl.multiple_of(slot * 8, 8), 8)], r2.at[j, own], s2.at[j, k], v2.at[j, own], dev)
        r2[j, own] = mid[j, pl.ds(pl.multiple_of(own * 8, 8), 8), :]
    for j in range(3):
        own_line = lines[j][0]
        own, others = planes[j]
        for k, (slot, dev) in enumerate(others):
            arrived(r2.at[j, slot], s2.at[j, k], v2.at[j, slot], dev)
        total = r2[j, 0]
        for q in range(1, 16):
            total = total + r2[j, q]
        spot = pl.ds(pl.multiple_of(mine + j * THIRD + own_line * 128 + own * 8, 8), 8)
        out_ref[spot, :] = total
        for k, (slot, dev) in enumerate(others):
            send(out_ref.at[spot], out_ref.at[spot], s3.at[j, k], v3.at[j, own], dev)
    for j in range(3):
        own_line, line = lines[j]
        own, others = planes[j]
        base = mine + j * THIRD + own_line * 128
        for k, (slot, dev) in enumerate(others):
            arrived(out_ref.at[pl.ds(pl.multiple_of(base + slot * 8, 8), 8)], s3.at[j, k], v3.at[j, slot], dev)
        spot = pl.ds(pl.multiple_of(base, 128), 128)
        for k, (slot, dev) in enumerate(line):
            send(out_ref.at[spot], out_ref.at[spot], s4.at[j, k], v4.at[j, own_line], dev)
        send(out_ref.at[spot], out_ref.at[spot], s5.at[j, 3], v5.at[j, own_line], mate)
    for j in range(3):
        own_line, line = lines[j]
        for k, (slot, dev) in enumerate(line):
            spot = pl.ds(pl.multiple_of(mine + j * THIRD + slot * 128, 128), 128)
            arrived(out_ref.at[spot], s4.at[j, k], v4.at[j, slot], dev)
            send(out_ref.at[spot], out_ref.at[spot], s5.at[j, k], v5.at[j, slot], mate)
    for j in range(3):
        for p in range(4):
            spot = pl.ds(pl.multiple_of(theirs + j * THIRD + p * 128, 128), 128)
            arrived(out_ref.at[spot], s5.at[j, 0], v5.at[j, p], mate)
    for c in pending:
        c.wait_send()


def run_total(part):
    vmem = pl.BlockSpec(memory_space=pltpu.VMEM)
    dma = pltpu.SemaphoreType.DMA
    f32 = jnp.float32
    return pl.pallas_call(
        total_kernel,
        out_shape=jax.ShapeDtypeStruct((PAD_K, 128), f32),
        in_specs=[vmem],
        out_specs=vmem,
        scratch_shapes=[
            pltpu.VMEM((3, THIRD, 128), f32),
            pltpu.VMEM((3, THIRD, 128), f32),
            pltpu.VMEM((3, 4, 128, 128), f32),
            pltpu.VMEM((3, 128, 128), f32),
            pltpu.VMEM((3, 16, 8, 128), f32),
            dma((3,)), dma((3,)), dma((3, 3)), dma((3, 4)), dma((3, 15)), dma((3, 16)),
            dma((3, 15)), dma((3, 16)), dma((3, 3)), dma((3, 4)), dma((3, 4)), dma((3, 4)),
        ],
        name="total",
        compiler_params=pltpu.CompilerParams(collective_id=1, has_side_effects=True),
    )(part)


def local_step(z_one, z_two, z_small, protos, live_mask):
    b, rows, live = run_codes(z_one, z_two, z_small, protos, live_mask[None, :])
    q_one, q_two, dz_one, dz_two, dz_small, part = run_grads(z_one, z_two, z_small, protos, b, rows, live)
    total = run_total(part)
    loss_total = -jnp.sum(total[NUM_K:NUM_K + 8]) / (live[0, 0] * 10.0)
    return q_one, q_two, loss_total, dz_one, dz_two, dz_small, total[:NUM_K]


def solution(mesh):
    row_spec = P("data", None)
    crop_spec = P(None, "data", None)
    return jax.shard_map(local_step, mesh=mesh,
                         in_specs=(row_spec, row_spec, crop_spec, P(None, None), P("data")),
                         out_specs=(row_spec, row_spec, P(), row_spec, row_spec, crop_spec, P(None, None)),
                         check_vma=False)
```

```python
import functools
import itertools

import jax
import jax.numpy as jnp
from jax import lax
from jax.experimental import pallas as pl
from jax.experimental.pallas import tpu as pltpu
from jax.sharding import PartitionSpec as P

EPS = 0.05
TAU = 0.1
ITERS = 3
LOG2E = 1.4426950408889634
ROWS = 256
NUM_K = 3000
PAD_K = 3072
TILES = PAD_K // 128
FULL = 11
CHUNK = 256
TAIL = NUM_K - FULL * CHUNK
VIEWS = 6
UNIT = 512

MESH = pl.DeviceIdType.MESH
STRIDE = {"x": 2, "y": 8, "z": 32}


def group_of(me, axes):
    pos = {a: lax.rem(lax.div(me, STRIDE[a]), 4) for a in axes}
    base = me
    own = 0
    for a in axes:
        base = base - pos[a] * STRIDE[a]
        own = own * 4 + pos[a]
    others = []
    for offs in itertools.product(range(4), repeat=len(axes)):
        if any(offs):
            slot, dev = 0, base
            for a, o in zip(axes, offs):
                q = lax.rem(pos[a] + o, 4)
                slot = slot * 4 + q
                dev = dev + q * STRIDE[a]
            others.append((slot, dev))
    return own, others


def enter(devs):
    bar = pltpu.get_barrier_semaphore()
    for d in devs:
        pl.semaphore_signal(bar, inc=1, device_id=(d,), device_id_type=MESH)
    return lambda: pl.semaphore_wait(bar, len(devs))


def codes_kernel(z1_ref, z2_ref, zs_ref, c_ref, m_ref, b_ref, rows_ref, live_ref, mix_ref, *rest):
    t_ref = rest[:VIEWS]
    (z_ref, zx, mcol, e, colsum, b8, dcol, drecv, slots_a, slots_b,
     zsend, zrecv, asend, arecv, bsend, brecv, fsend, frecv) = rest[VIEWS:]
    me = lax.axis_index("data")
    core = lax.rem(me, 2)
    mate = me + 1 - 2 * core
    own_a, others_a = group_of(me, "xy")
    own_b, others_b = group_of(me, "z")
    entered = enter([mate] + [d for _, d in others_a] + [d for _, d in others_b])

    z_ref[0] = z1_ref[...]
    z_ref[1] = z2_ref[...]
    mrow = jnp.broadcast_to(m_ref[...].astype(jnp.float32), (128, ROWS))
    mcol[0] = jnp.concatenate([mrow[:, :128].T, mrow[:, 128:].T], axis=0)

    def build(half, z_half):
        mk = mcol[half][:, :1]

        def piece(scores):
            return jnp.exp2(scores * (LOG2E / EPS)) * mk

        def step(i, carry):
            at = pl.multiple_of(i * CHUNK, CHUNK)
            s = lax.dot_general(z_half, c_ref[pl.ds(at, CHUNK), :], (((1,), (1,)), ((), ())),
                                preferred_element_type=jnp.float32)
            v = piece(s)
            e[pl.ds(half * ROWS, ROWS), pl.ds(at, CHUNK)] = v
            part = jnp.sum(v, axis=0, keepdims=True)
            if half:
                colsum[:, pl.ds(at, CHUNK)] += part
            else:
                colsum[:, pl.ds(at, CHUNK)] = part
            return carry

        lax.fori_loop(0, FULL, step, 0)
        s = lax.dot_general(z_half, c_ref[FULL * CHUNK:NUM_K, :], (((1,), (1,)), ((), ())),
                            preferred_element_type=jnp.float32)
        v = piece(s)
        e[half * ROWS:(half + 1) * ROWS, FULL * CHUNK + 128:] = jnp.zeros((ROWS, 128), jnp.float32)
        e[half * ROWS:(half + 1) * ROWS, FULL * CHUNK:NUM_K] = v
        part = jnp.sum(v, axis=0, keepdims=True)
        if half:
            colsum[:, FULL * CHUNK:NUM_K] += part
        else:
            colsum[:, FULL * CHUNK + 128:] = jnp.zeros((1, 128), jnp.float32)
            colsum[:, FULL * CHUNK:NUM_K] = part

    entered()
    give_z = pltpu.make_async_remote_copy(z_ref.at[1 - core], zx, zsend.at[0], zrecv.at[0],
                                          device_id=(mate,), device_id_type=MESH)
    give_m = pltpu.make_async_remote_copy(mcol.at[0], mcol.at[1], zsend.at[1], zrecv.at[1],
                                          device_id=(mate,), device_id_type=MESH)
    give_z.start()
    give_m.start()
    build(0, z_ref[core])
    give_z.wait()
    give_m.wait()
    build(1, zx[...])

    lane = lax.broadcasted_iota(jnp.int32, (1, 128), 1)
    flat = lax.broadcasted_iota(jnp.int32, (TILES, 128), 0) * 128 + lax.broadcasted_iota(jnp.int32, (TILES, 128), 1)
    count = jnp.sum(mcol[0] + mcol[1], axis=0, keepdims=True)

    mask = m_ref[...].astype(jnp.float32)

    def softmax_of(view):
        z_view = z_ref[view] if view < 2 else zs_ref[view - 2]

        def piece(at, n):
            s = lax.dot_general(c_ref[pl.ds(at, n), :], z_view, (((1,), (1,)), ((), ())),
                                preferred_element_type=jnp.float32)
            t = jnp.exp2(s * (LOG2E / TAU))
            t_ref[view][pl.ds(at, n), :] = t
            if view == 2:
                mix_ref[1, pl.ds(at, n), :] = s
            elif view == 0:
                mix_ref[0, pl.ds(at, n), :] = mix_ref[1, pl.ds(at, n), :] + s
            else:
                mix_ref[1, pl.ds(at, n), :] += s
            return jnp.sum(t.reshape(n // 8, 8, ROWS), axis=0)

        acc = lax.fori_loop(0, NUM_K // UNIT, lambda i, acc: acc + piece(pl.multiple_of(i * UNIT, UNIT), UNIT),
                            jnp.zeros((8, ROWS), jnp.float32))
        acc = acc + piece(NUM_K // UNIT * UNIT, NUM_K % UNIT)
        total = jnp.sum(acc, axis=0, keepdims=True)
        share = mask if view < 2 else 2.0 * mask
        rows_ref[2 + view:3 + view, :] = share / total
        lse = jnp.log(total) * share
        rows_ref[8:9, :] = lse if view == 2 else rows_ref[8:9, :] + lse

    def exchange(slots, send, recv, it, own, others, work):
        copies = []
        for k, (_, dev) in enumerate(others):
            copies.append(pltpu.make_async_remote_copy(
                slots.at[it, own], slots.at[it, own], send.at[it, k], recv.at[it, own],
                device_id=(dev,), device_id_type=MESH))
            copies[-1].start()
        work()
        for slot, dev in others:
            pltpu.make_async_remote_copy(
                slots.at[it, slot], slots.at[it, slot], send.at[it, 0], recv.at[it, slot],
                device_id=(dev,), device_id_type=MESH).wait_recv()
        total = slots[it, 0]
        for q in range(1, len(others) + 1):
            total = total + slots[it, q]
        return total, copies

    pending = []
    for it in range(ITERS):
        for t in range(TILES):
            row = colsum[:, t * 128:(t + 1) * 128]
            if it == 0 and t == TILES - 1:
                row = jnp.where(lane == NUM_K % 128, count, row)
            slots_a[it, own_a, t:t + 1, :] = row
        total, copies = exchange(slots_a, asend, arecv, it, own_a, others_a, functools.partial(softmax_of, (2, 4, 0)[it]))
        pending += copies
        slots_b[it, own_b] = total
        total, copies = exchange(slots_b, bsend, brecv, it, own_b, others_b, functools.partial(softmax_of, (3, 5, 1)[it]))
        pending += copies
        if it == 0:
            live_ref[...] = jnp.broadcast_to(total[TILES - 1:TILES, NUM_K % 128:NUM_K % 128 + 1], (8, 128))
        inside = flat < NUM_K
        bmat = jnp.where(inside, 1.0 / (NUM_K * jnp.where(inside, total, 1.0)), 0.0)
        if it == ITERS - 1:
            b_ref[core] = bmat
            give_b = pltpu.make_async_remote_copy(b_ref.at[core], b_ref.at[core], fsend.at[0], frecv.at[0],
                                                  device_id=(mate,), device_id_type=MESH)
            give_b.start()
        for t in range(TILES):
            b8[:, t * 128:(t + 1) * 128] = jnp.broadcast_to(bmat[t:t + 1, :], (8, 128))
        if it < ITERS - 1:
            colsum[...] = jnp.zeros_like(colsum)

        def block(i, carry):
            r0 = pl.multiple_of(i * 128, 128)
            acc = jnp.zeros((128, 128), jnp.float32)
            for t in range(TILES):
                acc += (e[pl.ds(r0, 128), t * 128:(t + 1) * 128].reshape(16, 8, 128)
                        * b8[:, t * 128:(t + 1) * 128][None]).reshape(128, 128)
            d = jnp.sum(acc, axis=1, keepdims=True)
            a = jnp.where(d > 0, 1.0 / jnp.where(d > 0, d, 1.0), 0.0)
            if it == ITERS - 1:
                dcol[pl.ds(r0, 128), :] = jnp.broadcast_to(a, (128, 128))
            else:
                ab = jnp.broadcast_to(a, (128, 128))
                for t in range(TILES):
                    colsum[:, t * 128:(t + 1) * 128] += jnp.sum(
                        e[pl.ds(r0, 128), t * 128:(t + 1) * 128] * ab, axis=0, keepdims=True)
            return carry

        lax.fori_loop(0, 2 * ROWS // 128, block, 0)

    give_a = pltpu.make_async_remote_copy(dcol.at[pl.ds(ROWS, ROWS)], drecv, fsend.at[1], frecv.at[1],
                                          device_id=(mate,), device_id_type=MESH)
    give_a.start()
    for c in pending:
        c.wait_send()
    give_b.wait_send()
    pltpu.make_async_remote_copy(b_ref.at[1 - core], b_ref.at[1 - core], fsend.at[0], frecv.at[0],
                                 device_id=(mate,), device_id_type=MESH).wait_recv()
    give_a.wait()
    first = core == 0
    own_r = jnp.concatenate([dcol[:128, :].T, dcol[128:ROWS, :].T], axis=1)[:1]
    mate_r = jnp.concatenate([drecv[:128, :].T, drecv[128:, :].T], axis=1)[:1]
    rows_ref[0:1, :] = jnp.where(first, own_r, mate_r)
    rows_ref[1:2, :] = jnp.where(first, mate_r, own_r)


def run_codes(z_one, z_two, z_small, protos, mask_row):
    vmem = pl.BlockSpec(memory_space=pltpu.VMEM)
    dma = pltpu.SemaphoreType.DMA
    return pl.pallas_call(
        codes_kernel,
        out_shape=(pltpu.VMEM((2, TILES, 128), jnp.float32),
                   pltpu.VMEM((16, ROWS), jnp.float32),
                   pltpu.VMEM((8, 128), jnp.float32),
                   pltpu.VMEM((2, NUM_K, ROWS), jnp.float32),
                   *[pltpu.VMEM((NUM_K, ROWS), jnp.float32)] * VIEWS),
        in_specs=[vmem] * 5,
        out_specs=(vmem,) * (4 + VIEWS),
        scratch_shapes=[
            pltpu.VMEM((2, ROWS, 128), jnp.bfloat16),
            pltpu.VMEM((ROWS, 128), jnp.bfloat16),
            pltpu.VMEM((2, ROWS, 128), jnp.float32),
            pltpu.VMEM((2 * ROWS, PAD_K), jnp.float32),
            pltpu.VMEM((1, PAD_K), jnp.float32),
            pltpu.VMEM((8, PAD_K), jnp.float32),
            pltpu.VMEM((2 * ROWS, 128), jnp.float32),
            pltpu.VMEM((ROWS, 128), jnp.float32),
            pltpu.VMEM((ITERS, 16, TILES, 128), jnp.float32),
            pltpu.VMEM((ITERS, 4, TILES, 128), jnp.float32),
            dma((2,)), dma((2,)),
            dma((ITERS, 15)), dma((ITERS, 16)),
            dma((ITERS, 3)), dma((ITERS, 4)),
            dma((2,)), dma((2,)),
        ],
        name="codes",
        compiler_params=pltpu.CompilerParams(collective_id=0, has_side_effects=True, vmem_limit_bytes=26 << 20),
    )(z_one, z_two, z_small, protos, mask_row)


KC = 1000
STEPS = NUM_K // KC
RB = 8
UNROLL = 5


def grads_kernel(z1_ref, z2_ref, zs_ref, c_ref, b_ref, rows_ref, live_ref, mix_ref, *rest):
    t_ref = rest[:VIEWS]
    (q1_ref, q2_ref, dz1_ref, dz2_ref, dzs_ref, dc_ref, loss_ref,
     zall, g_all, dz_acc, loss_acc, rvec, bcol) = rest[VIEWS:]
    i = pl.program_id(0)
    g = 1.0 / (TAU * 10.0 * live_ref[0:1, 0:1])

    @pl.when(i == 0)
    def _():
        zall[0:ROWS] = z1_ref[...]
        zall[ROWS:2 * ROWS] = z2_ref[...]
        for j in range(4):
            zall[(2 + j) * ROWS:(3 + j) * ROWS] = zs_ref[j]
        dz_acc[...] = jnp.zeros_like(dz_acc)
        loss_acc[...] = jnp.zeros_like(loss_acc)
        for v in range(2 + VIEWS):
            rvec[v] = jnp.broadcast_to(rows_ref[v:v + 1, :] * (1.0 if v < 2 else g), (8, ROWS))
        for v in range(2):
            for t in range(TILES // 8):
                bt = jnp.concatenate([b_ref[v, t * 8:(t + 1) * 8, :]] * 16, axis=0).T
                for k in range(8):
                    at = (t * 8 + k) * 128
                    bcol[v, at:at + 128, :] = jnp.broadcast_to(bt[:, k:k + 1], (128, 128))

    def block(n, acc):
        at = pl.multiple_of(n * RB, RB)
        src = pl.multiple_of(i * KC + n * RB, RB)
        t = [t_ref[v][pl.ds(src, RB), :] for v in range(VIEWS)]
        b = [jnp.concatenate([bcol[v, pl.ds(src, RB), :]] * 2, axis=1) for v in range(2)]
        q1 = (t[0] * rvec[0]) * (t[0] * b[0])
        q2 = (t[1] * rvec[1]) * (t[1] * b[1])
        q1_ref[pl.ds(at, RB), :] = q1
        q2_ref[pl.ds(at, RB), :] = q2
        term = q2 * mix_ref[0, pl.ds(src, RB), :] + q1 * mix_ref[1, pl.ds(src, RB), :]
        gq1 = q1 * g
        gq2 = q2 * g
        gqs = gq1 + gq2
        for v in range(VIEWS):
            sub = (gq2, gq1)[v] if v < 2 else gqs
            g_all[pl.ds(at, RB), v * ROWS:(v + 1) * ROWS] = (t[v] * rvec[2 + v] - sub).astype(jnp.bfloat16)
        return acc + term[:, :128] + term[:, 128:]

    loss_acc[...] = lax.fori_loop(0, KC // RB, block, loss_acc[...], unroll=UNROLL)
    dz_acc[...] += lax.dot_general(g_all[...], c_ref[...], (((0,), (0,)), ((), ())), preferred_element_type=jnp.float32)
    dc_ref[...] = lax.dot_general(g_all[...], zall[...], (((1,), (0,)), ((), ())), preferred_element_type=jnp.float32)

    @pl.when(i == STEPS - 1)
    def _():
        dz1_ref[...] = dz_acc[0:ROWS]
        dz2_ref[...] = dz_acc[ROWS:2 * ROWS]
        for j in range(4):
            dzs_ref[j] = dz_acc[(2 + j) * ROWS:(3 + j) * ROWS]
        lse = jnp.sum(rows_ref[8:9, :])
        lane0 = ((lax.broadcasted_iota(jnp.int32, (8, 128), 0) == 0)
                 & (lax.broadcasted_iota(jnp.int32, (8, 128), 1) == 0))
        loss_ref[...] = loss_acc[...] * (1.0 / TAU) - jnp.where(lane0, lse, 0.0)


def run_grads(z_one, z_two, z_small, protos, b, rows, live, mix, t):
    def whole(*shape):
        return pl.BlockSpec(shape, lambda i: (0,) * len(shape))

    f32 = jnp.float32
    vmem = pl.BlockSpec(memory_space=pltpu.VMEM)
    return pl.pallas_call(
        grads_kernel,
        grid=(STEPS,),
        out_shape=(jax.ShapeDtypeStruct((NUM_K, ROWS), f32), jax.ShapeDtypeStruct((NUM_K, ROWS), f32),
                   jax.ShapeDtypeStruct((ROWS, 128), f32), jax.ShapeDtypeStruct((ROWS, 128), f32),
                   jax.ShapeDtypeStruct((4, ROWS, 128), f32), jax.ShapeDtypeStruct((NUM_K, 128), f32),
                   jax.ShapeDtypeStruct((8, 128), f32)),
        in_specs=[whole(ROWS, 128), whole(ROWS, 128), whole(4, ROWS, 128),
                  pl.BlockSpec((KC, 128), lambda i: (i, 0)), vmem, vmem, vmem, vmem] + [vmem] * VIEWS,
        out_specs=(pl.BlockSpec((KC, ROWS), lambda i: (i, 0)), pl.BlockSpec((KC, ROWS), lambda i: (i, 0)),
                   whole(ROWS, 128), whole(ROWS, 128), whole(4, ROWS, 128),
                   pl.BlockSpec((KC, 128), lambda i: (i, 0)), whole(8, 128)),
        scratch_shapes=[
            pltpu.VMEM((VIEWS * ROWS, 128), jnp.bfloat16),
            pltpu.VMEM((KC, VIEWS * ROWS), jnp.bfloat16),
            pltpu.VMEM((VIEWS * ROWS, 128), f32),
            pltpu.VMEM((8, 128), f32),
            pltpu.VMEM((2 + VIEWS, 8, ROWS), f32),
            pltpu.VMEM((2, PAD_K, 128), f32),
        ],
        name="grads",
        compiler_params=pltpu.CompilerParams(dimension_semantics=("arbitrary",), vmem_limit_bytes=26 << 20),
    )(z_one, z_two, z_small, protos, b, rows, live, mix, *t)


HALF = PAD_K // 2
THIRD = HALF // 3
ORDERS = (("x", "yz"), ("y", "xz"), ("z", "xy"))


def total_kernel(dc_ref, loss_ref, dout_ref, lout_ref, part_ref, out_ref, r0, acc, r1, mid, r2,
                 s0, v0, s1, v1, s2, v2, s3, v3, s4, v4, s5, v5):
    me = lax.axis_index("data")
    core = lax.rem(me, 2)
    mate = me + 1 - 2 * core
    lines = [group_of(me, a) for a, _ in ORDERS]
    planes = [group_of(me, p) for _, p in ORDERS]
    devs = [mate]
    for _, others in lines:
        devs += [d for _, d in others]
    for n, (_, others) in enumerate(planes):
        axes = ORDERS[n][1]
        devs += [d for (_, d), offs in zip(others, [o for o in itertools.product(range(4), repeat=2) if any(o)]) if all(offs)]
    part_ref[:NUM_K, :] = dc_ref[...]
    part_ref[NUM_K:NUM_K + 8, :] = loss_ref[...]
    part_ref[NUM_K + 8:, :] = jnp.zeros((PAD_K - NUM_K - 8, 128), jnp.float32)
    enter(devs)()
    mine = pl.multiple_of(core * HALF, HALF)
    theirs = pl.multiple_of((1 - core) * HALF, HALF)
    pending = []

    def send(src, dst, ssem, rsem, dev):
        c = pltpu.make_async_remote_copy(src, dst, ssem, rsem, device_id=(dev,), device_id_type=MESH)
        c.start()
        pending.append(c)

    def arrived(dst, ssem, rsem, dev):
        pltpu.make_async_remote_copy(dst, dst, ssem, rsem, device_id=(dev,), device_id_type=MESH).wait_recv()

    for j in range(3):
        send(part_ref.at[pl.ds(theirs + j * THIRD, THIRD)], r0.at[j], s0.at[j], v0.at[j], mate)
    for j in range(3):
        arrived(r0.at[j], s0.at[j], v0.at[j], mate)
        acc[j] = part_ref[pl.ds(mine + j * THIRD, THIRD), :] + r0[j]
        own, others = lines[j]
        for k, (slot, dev) in enumerate(others):
            send(acc.at[j, pl.ds(pl.multiple_of(slot * 128, 128), 128)], r1.at[j, own], s1.at[j, k], v1.at[j, own], dev)
        r1[j, own] = acc[j, pl.ds(pl.multiple_of(own * 128, 128), 128), :]
    for j in range(3):
        own, others = lines[j]
        for k, (slot, dev) in enumerate(others):
            arrived(r1.at[j, slot], s1.at[j, k], v1.at[j, slot], dev)
        mid[j] = (r1[j, 0] + r1[j, 1]) + (r1[j, 2] + r1[j, 3])
        own, others = planes[j]
        for k, (slot, dev) in enumerate(others):
            send(mid.at[j, pl.ds(pl.multiple_of(slot * 8, 8), 8)], r2.at[j, own], s2.at[j, k], v2.at[j, own], dev)
        r2[j, own] = mid[j, pl.ds(pl.multiple_of(own * 8, 8), 8), :]
    for j in range(3):
        own_line = lines[j][0]
        own, others = planes[j]
        for k, (slot, dev) in enumerate(others):
            arrived(r2.at[j, slot], s2.at[j, k], v2.at[j, slot], dev)
        total = r2[j, 0]
        for q in range(1, 16):
            total = total + r2[j, q]
        spot = pl.ds(pl.multiple_of(mine + j * THIRD + own_line * 128 + own * 8, 8), 8)
        out_ref[spot, :] = total
        for k, (slot, dev) in enumerate(others):
            send(out_ref.at[spot], out_ref.at[spot], s3.at[j, k], v3.at[j, own], dev)
    for j in range(3):
        own_line, line = lines[j]
        own, others = planes[j]
        base = mine + j * THIRD + own_line * 128
        for k, (slot, dev) in enumerate(others):
            arrived(out_ref.at[pl.ds(pl.multiple_of(base + slot * 8, 8), 8)], s3.at[j, k], v3.at[j, slot], dev)
        spot = pl.ds(pl.multiple_of(base, 128), 128)
        for k, (slot, dev) in enumerate(line):
            send(out_ref.at[spot], out_ref.at[spot], s4.at[j, k], v4.at[j, own_line], dev)
        send(out_ref.at[spot], out_ref.at[spot], s5.at[j, 3], v5.at[j, own_line], mate)
    for j in range(3):
        own_line, line = lines[j]
        for k, (slot, dev) in enumerate(line):
            spot = pl.ds(pl.multiple_of(mine + j * THIRD + slot * 128, 128), 128)
            arrived(out_ref.at[spot], s4.at[j, k], v4.at[j, slot], dev)
            send(out_ref.at[spot], out_ref.at[spot], s5.at[j, k], v5.at[j, slot], mate)
    for j in range(3):
        for p in range(4):
            spot = pl.ds(pl.multiple_of(theirs + j * THIRD + p * 128, 128), 128)
            arrived(out_ref.at[spot], s5.at[j, 0], v5.at[j, p], mate)
    dout_ref[...] = out_ref[:NUM_K, :]
    lout_ref[...] = out_ref[NUM_K:NUM_K + 8, :]
    for c in pending:
        c.wait_send()


def run_total(part, loss):
    vmem = pl.BlockSpec(memory_space=pltpu.VMEM)
    dma = pltpu.SemaphoreType.DMA
    f32 = jnp.float32
    return pl.pallas_call(
        total_kernel,
        out_shape=(jax.ShapeDtypeStruct((NUM_K, 128), f32), jax.ShapeDtypeStruct((8, 128), f32)),
        in_specs=[vmem, vmem],
        out_specs=(vmem, vmem),
        scratch_shapes=[
            pltpu.VMEM((PAD_K, 128), f32),
            pltpu.VMEM((PAD_K, 128), f32),
            pltpu.VMEM((3, THIRD, 128), f32),
            pltpu.VMEM((3, THIRD, 128), f32),
            pltpu.VMEM((3, 4, 128, 128), f32),
            pltpu.VMEM((3, 128, 128), f32),
            pltpu.VMEM((3, 16, 8, 128), f32),
            dma((3,)), dma((3,)), dma((3, 3)), dma((3, 4)), dma((3, 15)), dma((3, 16)),
            dma((3, 15)), dma((3, 16)), dma((3, 3)), dma((3, 4)), dma((3, 4)), dma((3, 4)),
        ],
        name="total",
        compiler_params=pltpu.CompilerParams(collective_id=1, has_side_effects=True, vmem_limit_bytes=16 << 20),
    )(part, loss)


def local_step(z_one, z_two, z_small, protos, live_mask):
    b, rows, live, mix, *t = run_codes(z_one, z_two, z_small, protos, live_mask[None, :])
    q_one, q_two, dz_one, dz_two, dz_small, part, loss = run_grads(
        z_one, z_two, z_small, protos, b, rows, live, mix, t)
    total, loss_sum = run_total(part, loss)
    loss_total = -jnp.sum(loss_sum) / (live[0, 0] * 10.0)
    return q_one.T, q_two.T, loss_total, dz_one, dz_two, dz_small, total


def solution(mesh):
    row_spec = P("data", None)
    crop_spec = P(None, "data", None)
    return jax.shard_map(local_step, mesh=mesh,
                         in_specs=(row_spec, row_spec, crop_spec, P(None, None), P("data")),
                         out_specs=(row_spec, row_spec, P(), row_spec, row_spec, crop_spec, P(None, None)),
                         check_vma=False)
```

```python
import functools
import itertools

import jax
import jax.numpy as jnp
from jax import lax
from jax.experimental import pallas as pl
from jax.experimental.pallas import tpu as pltpu
from jax.sharding import PartitionSpec as P

EPS = 0.05
TAU = 0.1
ITERS = 3
LOG2E = 1.4426950408889634
ROWS = 256
NUM_K = 3000
PAD_K = 3072
TILES = PAD_K // 128
CHUNK = 512
FULL = NUM_K // CHUNK
TAIL = NUM_K - FULL * CHUNK
VIEWS = 6
UNIT = 512

MESH = pl.DeviceIdType.MESH
STRIDE = {"x": 2, "y": 8, "z": 32}


def group_of(me, axes):
    pos = {a: lax.rem(lax.div(me, STRIDE[a]), 4) for a in axes}
    base = me
    own = 0
    for a in axes:
        base = base - pos[a] * STRIDE[a]
        own = own * 4 + pos[a]
    others = []
    for offs in itertools.product(range(4), repeat=len(axes)):
        if any(offs):
            slot, dev = 0, base
            for a, o in zip(axes, offs):
                q = lax.rem(pos[a] + o, 4)
                slot = slot * 4 + q
                dev = dev + q * STRIDE[a]
            others.append((slot, dev))
    return own, others


def enter(devs):
    bar = pltpu.get_barrier_semaphore()
    for d in devs:
        pl.semaphore_signal(bar, inc=1, device_id=(d,), device_id_type=MESH)
    return lambda: pl.semaphore_wait(bar, len(devs))


def codes_kernel(z1_hbm, z2_hbm, zs_hbm, c_hbm, m_hbm, b_ref, rows_ref, live_ref, z_ref, c_ref, mix_ref, *rest):
    t_ref = rest[:VIEWS]
    (m_ref, insem, zx, mcol, e, colsum, b8, dcol, drecv, slots_a, slots_b,
     zsend, zrecv, asend, arecv, bsend, brecv, fsend, frecv) = rest[VIEWS:]
    me = lax.axis_index("data")
    core = lax.rem(me, 2)
    mate = me + 1 - 2 * core
    own_a, others_a = group_of(me, "xy")
    own_b, others_b = group_of(me, "z")
    entered = enter([mate] + [d for _, d in others_a] + [d for _, d in others_b])

    loads = [pltpu.make_async_copy(m_hbm, m_ref, insem.at[0]),
             pltpu.make_async_copy(z1_hbm, z_ref.at[0], insem.at[1]),
             pltpu.make_async_copy(z2_hbm, z_ref.at[1], insem.at[2]),
             pltpu.make_async_copy(c_hbm, c_ref, insem.at[3]),
             pltpu.make_async_copy(zs_hbm, z_ref.at[pl.ds(2, 4)], insem.at[4])]
    for c in loads:
        c.start()
    for c in loads:
        c.wait()
    mrow = jnp.broadcast_to(m_ref[...].astype(jnp.float32), (128, ROWS))
    mcol[0] = jnp.concatenate([mrow[:, :128].T, mrow[:, 128:].T], axis=0)

    def build(half, z_half):
        mk = mcol[half][:, :1]

        def piece(scores):
            return jnp.exp2(scores * (LOG2E / EPS)) * mk

        def step(i, carry):
            at = pl.multiple_of(i * CHUNK, CHUNK)
            s = lax.dot_general(z_half, c_ref[pl.ds(at, CHUNK), :], (((1,), (1,)), ((), ())),
                                preferred_element_type=jnp.float32)
            v = piece(s)
            e[pl.ds(half * ROWS, ROWS), pl.ds(at, CHUNK)] = v
            part = jnp.sum(v, axis=0, keepdims=True)
            if half:
                colsum[:, pl.ds(at, CHUNK)] += part
            else:
                colsum[:, pl.ds(at, CHUNK)] = part
            return carry

        lax.fori_loop(0, FULL, step, 0)
        s = lax.dot_general(z_half, c_ref[FULL * CHUNK:NUM_K, :], (((1,), (1,)), ((), ())),
                            preferred_element_type=jnp.float32)
        v = piece(s)
        e[half * ROWS:(half + 1) * ROWS, NUM_K // 128 * 128:] = jnp.zeros((ROWS, 128), jnp.float32)
        e[half * ROWS:(half + 1) * ROWS, FULL * CHUNK:NUM_K] = v
        part = jnp.sum(v, axis=0, keepdims=True)
        if half:
            colsum[:, FULL * CHUNK:NUM_K] += part
        else:
            colsum[:, NUM_K // 128 * 128:] = jnp.zeros((1, 128), jnp.float32)
            colsum[:, FULL * CHUNK:NUM_K] = part

    entered()
    give_z = pltpu.make_async_remote_copy(z_ref.at[1 - core], zx, zsend.at[0], zrecv.at[0],
                                          device_id=(mate,), device_id_type=MESH)
    give_m = pltpu.make_async_remote_copy(mcol.at[0], mcol.at[1], zsend.at[1], zrecv.at[1],
                                          device_id=(mate,), device_id_type=MESH)
    give_z.start()
    give_m.start()
    build(0, z_ref[core])
    give_z.wait()
    give_m.wait()
    build(1, zx[...])

    lane = lax.broadcasted_iota(jnp.int32, (1, 128), 1)
    flat = lax.broadcasted_iota(jnp.int32, (TILES, 128), 0) * 128 + lax.broadcasted_iota(jnp.int32, (TILES, 128), 1)
    count = jnp.sum(mcol[0] + mcol[1], axis=0, keepdims=True)

    mask = m_ref[...].astype(jnp.float32)

    def softmax_of(view):
        z_view = z_ref[view]

        def piece(at, n):
            s = lax.dot_general(c_ref[pl.ds(at, n), :], z_view, (((1,), (1,)), ((), ())),
                                preferred_element_type=jnp.float32)
            t = jnp.exp2(s * (LOG2E / TAU))
            t_ref[view][pl.ds(at, n), :] = t
            if view == 2:
                mix_ref[1, pl.ds(at, n), :] = s
            elif view == 0:
                mix_ref[0, pl.ds(at, n), :] = mix_ref[1, pl.ds(at, n), :] + s
            else:
                mix_ref[1, pl.ds(at, n), :] += s
            return jnp.sum(t.reshape(n // 8, 8, ROWS), axis=0)

        acc = lax.fori_loop(0, NUM_K // UNIT, lambda i, acc: acc + piece(pl.multiple_of(i * UNIT, UNIT), UNIT),
                            jnp.zeros((8, ROWS), jnp.float32))
        acc = acc + piece(NUM_K // UNIT * UNIT, NUM_K % UNIT)
        total = jnp.sum(acc, axis=0, keepdims=True)
        share = mask if view < 2 else 2.0 * mask
        rows_ref[2 + view:3 + view, :] = share / total
        lse = jnp.log(total) * share
        rows_ref[8:9, :] = lse if view == 2 else rows_ref[8:9, :] + lse

    def exchange(slots, send, recv, it, own, others, work):
        copies = []
        for k, (_, dev) in enumerate(others):
            copies.append(pltpu.make_async_remote_copy(
                slots.at[it, own], slots.at[it, own], send.at[it, k], recv.at[it, own],
                device_id=(dev,), device_id_type=MESH))
            copies[-1].start()
        work()
        for slot, dev in others:
            pltpu.make_async_remote_copy(
                slots.at[it, slot], slots.at[it, slot], send.at[it, 0], recv.at[it, slot],
                device_id=(dev,), device_id_type=MESH).wait_recv()
        total = slots[it, 0]
        for q in range(1, len(others) + 1):
            total = total + slots[it, q]
        return total, copies

    pending = []
    for it in range(ITERS):
        for t in range(TILES):
            row = colsum[:, t * 128:(t + 1) * 128]
            if it == 0 and t == TILES - 1:
                row = jnp.where(lane == NUM_K % 128, count, row)
            slots_a[it, own_a, t:t + 1, :] = row
        total, copies = exchange(slots_a, asend, arecv, it, own_a, others_a, functools.partial(softmax_of, (2, 4, 0)[it]))
        pending += copies
        slots_b[it, own_b] = total
        total, copies = exchange(slots_b, bsend, brecv, it, own_b, others_b, functools.partial(softmax_of, (3, 5, 1)[it]))
        pending += copies
        if it == 0:
            live_ref[...] = jnp.broadcast_to(total[TILES - 1:TILES, NUM_K % 128:NUM_K % 128 + 1], (8, 128))
        inside = flat < NUM_K
        bmat = jnp.where(inside, 1.0 / (NUM_K * jnp.where(inside, total, 1.0)), 0.0)
        if it == ITERS - 1:
            b_ref[core] = bmat
            give_b = pltpu.make_async_remote_copy(b_ref.at[core], b_ref.at[core], fsend.at[0], frecv.at[0],
                                                  device_id=(mate,), device_id_type=MESH)
            give_b.start()
        for t in range(TILES):
            b8[:, t * 128:(t + 1) * 128] = jnp.broadcast_to(bmat[t:t + 1, :], (8, 128))
        if it < ITERS - 1:
            colsum[...] = jnp.zeros_like(colsum)

        def block(i, carry):
            r0 = pl.multiple_of(i * 128, 128)
            acc = jnp.zeros((128, 128), jnp.float32)
            for t in range(TILES):
                acc += (e[pl.ds(r0, 128), t * 128:(t + 1) * 128].reshape(16, 8, 128)
                        * b8[:, t * 128:(t + 1) * 128][None]).reshape(128, 128)
            d = jnp.sum(acc, axis=1, keepdims=True)
            a = jnp.where(d > 0, 1.0 / jnp.where(d > 0, d, 1.0), 0.0)
            if it == ITERS - 1:
                dcol[pl.ds(r0, 128), :] = jnp.broadcast_to(a, (128, 128))
            else:
                ab = jnp.broadcast_to(a, (128, 128))
                for t in range(TILES):
                    colsum[:, t * 128:(t + 1) * 128] += jnp.sum(
                        e[pl.ds(r0, 128), t * 128:(t + 1) * 128] * ab, axis=0, keepdims=True)
            return carry

        lax.fori_loop(0, 2 * ROWS // 128, block, 0)

    give_a = pltpu.make_async_remote_copy(dcol.at[pl.ds(ROWS, ROWS)], drecv, fsend.at[1], frecv.at[1],
                                          device_id=(mate,), device_id_type=MESH)
    give_a.start()
    for c in pending:
        c.wait_send()
    give_b.wait_send()
    pltpu.make_async_remote_copy(b_ref.at[1 - core], b_ref.at[1 - core], fsend.at[0], frecv.at[0],
                                 device_id=(mate,), device_id_type=MESH).wait_recv()
    give_a.wait()
    first = core == 0
    own_r = jnp.concatenate([dcol[:128, :].T, dcol[128:ROWS, :].T], axis=1)[:1]
    mate_r = jnp.concatenate([drecv[:128, :].T, drecv[128:, :].T], axis=1)[:1]
    rows_ref[0:1, :] = jnp.where(first, own_r, mate_r)
    rows_ref[1:2, :] = jnp.where(first, mate_r, own_r)


def run_codes(z_one, z_two, z_small, protos, mask_row):
    hbm = pl.BlockSpec(memory_space=pltpu.HBM)
    vmem = pl.BlockSpec(memory_space=pltpu.VMEM)
    dma = pltpu.SemaphoreType.DMA
    return pl.pallas_call(
        codes_kernel,
        out_shape=(pltpu.VMEM((2, TILES, 128), jnp.float32),
                   pltpu.VMEM((16, ROWS), jnp.float32),
                   pltpu.VMEM((8, 128), jnp.float32),
                   pltpu.VMEM((VIEWS, ROWS, 128), jnp.bfloat16),
                   pltpu.VMEM((NUM_K, 128), jnp.bfloat16),
                   pltpu.VMEM((2, NUM_K, ROWS), jnp.float32),
                   *[pltpu.VMEM((NUM_K, ROWS), jnp.float32)] * VIEWS),
        in_specs=[hbm] * 5,
        out_specs=(vmem,) * (6 + VIEWS),
        scratch_shapes=[
            pltpu.VMEM((1, ROWS), jnp.int32),
            dma((5,)),
            pltpu.VMEM((ROWS, 128), jnp.bfloat16),
            pltpu.VMEM((2, ROWS, 128), jnp.float32),
            pltpu.VMEM((2 * ROWS, PAD_K), jnp.float32),
            pltpu.VMEM((1, PAD_K), jnp.float32),
            pltpu.VMEM((8, PAD_K), jnp.float32),
            pltpu.VMEM((2 * ROWS, 128), jnp.float32),
            pltpu.VMEM((ROWS, 128), jnp.float32),
            pltpu.VMEM((ITERS, 16, TILES, 128), jnp.float32),
            pltpu.VMEM((ITERS, 4, TILES, 128), jnp.float32),
            dma((2,)), dma((2,)),
            dma((ITERS, 15)), dma((ITERS, 16)),
            dma((ITERS, 3)), dma((ITERS, 4)),
            dma((2,)), dma((2,)),
        ],
        name="codes",
        compiler_params=pltpu.CompilerParams(collective_id=0, has_side_effects=True, vmem_limit_bytes=26 << 20),
    )(*[pltpu.with_memory_space_constraint(x, pltpu.HBM) for x in (z_one, z_two, z_small, protos, mask_row)])


KC = 1000
STEPS = NUM_K // KC
RB = 8
UNROLL = 5


def grads_kernel(z_ref, c_ref, b_ref, rows_ref, live_ref, mix_ref, *rest):
    t_ref = rest[:VIEWS]
    (q1_ref, q2_ref, dz1_ref, dz2_ref, dzs_ref, dc_ref, loss_ref,
     g_all, dz_acc, loss_acc, rvec, bcol) = rest[VIEWS:]
    i = pl.program_id(0)
    g = 1.0 / (TAU * 10.0 * live_ref[0:1, 0:1])

    @pl.when(i == 0)
    def _():
        dz_acc[...] = jnp.zeros_like(dz_acc)
        loss_acc[...] = jnp.zeros_like(loss_acc)
        for v in range(2 + VIEWS):
            rvec[v] = jnp.broadcast_to(rows_ref[v:v + 1, :] * (1.0 if v < 2 else g), (8, ROWS))
        for v in range(2):
            for t in range(TILES // 8):
                bt = jnp.concatenate([b_ref[v, t * 8:(t + 1) * 8, :]] * 16, axis=0).T
                for k in range(8):
                    at = (t * 8 + k) * 128
                    bcol[v, at:at + 128, :] = jnp.broadcast_to(bt[:, k:k + 1], (128, 128))

    def block(n, acc):
        at = pl.multiple_of(n * RB, RB)
        src = pl.multiple_of(i * KC + n * RB, RB)
        t = [t_ref[v][pl.ds(src, RB), :] for v in range(VIEWS)]
        b = [jnp.concatenate([bcol[v, pl.ds(src, RB), :]] * 2, axis=1) for v in range(2)]
        q1 = (t[0] * rvec[0]) * (t[0] * b[0])
        q2 = (t[1] * rvec[1]) * (t[1] * b[1])
        q1_ref[pl.ds(at, RB), :] = q1
        q2_ref[pl.ds(at, RB), :] = q2
        term = q2 * mix_ref[0, pl.ds(src, RB), :] + q1 * mix_ref[1, pl.ds(src, RB), :]
        gq1 = q1 * g
        gq2 = q2 * g
        gqs = gq1 + gq2
        for v in range(VIEWS):
            sub = (gq2, gq1)[v] if v < 2 else gqs
            g_all[pl.ds(at, RB), v * ROWS:(v + 1) * ROWS] = (t[v] * rvec[2 + v] - sub).astype(jnp.bfloat16)
        return acc + term[:, :128] + term[:, 128:]

    loss_acc[...] = lax.fori_loop(0, KC // RB, block, loss_acc[...], unroll=UNROLL)
    zall = z_ref[...].reshape(VIEWS * ROWS, 128)
    c_part = c_ref[pl.ds(pl.multiple_of(i * KC, 8), KC), :]
    dz_acc[...] += lax.dot_general(g_all[...], c_part, (((0,), (0,)), ((), ())), preferred_element_type=jnp.float32)
    dc_ref[...] = lax.dot_general(g_all[...], zall, (((1,), (0,)), ((), ())), preferred_element_type=jnp.float32)

    @pl.when(i == STEPS - 1)
    def _():
        dz1_ref[...] = dz_acc[0:ROWS]
        dz2_ref[...] = dz_acc[ROWS:2 * ROWS]
        for j in range(4):
            dzs_ref[j] = dz_acc[(2 + j) * ROWS:(3 + j) * ROWS]
        lse = jnp.sum(rows_ref[8:9, :])
        lane0 = ((lax.broadcasted_iota(jnp.int32, (8, 128), 0) == 0)
                 & (lax.broadcasted_iota(jnp.int32, (8, 128), 1) == 0))
        loss_ref[...] = loss_acc[...] * (1.0 / TAU) - jnp.where(lane0, lse, 0.0)


def run_grads(z, c, b, rows, live, mix, t):
    def whole(*shape):
        return pl.BlockSpec(shape, lambda i: (0,) * len(shape))

    f32 = jnp.float32
    vmem = pl.BlockSpec(memory_space=pltpu.VMEM)
    return pl.pallas_call(
        grads_kernel,
        grid=(STEPS,),
        out_shape=(jax.ShapeDtypeStruct((NUM_K, ROWS), f32), jax.ShapeDtypeStruct((NUM_K, ROWS), f32),
                   jax.ShapeDtypeStruct((ROWS, 128), f32), jax.ShapeDtypeStruct((ROWS, 128), f32),
                   jax.ShapeDtypeStruct((4, ROWS, 128), f32), jax.ShapeDtypeStruct((NUM_K, 128), f32),
                   jax.ShapeDtypeStruct((8, 128), f32)),
        in_specs=[vmem] * (6 + VIEWS),
        out_specs=(pl.BlockSpec((KC, ROWS), lambda i: (i, 0)), pl.BlockSpec((KC, ROWS), lambda i: (i, 0)),
                   whole(ROWS, 128), whole(ROWS, 128), whole(4, ROWS, 128),
                   pl.BlockSpec((KC, 128), lambda i: (i, 0)), whole(8, 128)),
        scratch_shapes=[
            pltpu.VMEM((KC, VIEWS * ROWS), jnp.bfloat16),
            pltpu.VMEM((VIEWS * ROWS, 128), f32),
            pltpu.VMEM((8, 128), f32),
            pltpu.VMEM((2 + VIEWS, 8, ROWS), f32),
            pltpu.VMEM((2, PAD_K, 128), f32),
        ],
        name="grads",
        compiler_params=pltpu.CompilerParams(dimension_semantics=("arbitrary",), vmem_limit_bytes=26 << 20),
    )(z, c, b, rows, live, mix, *t)


HALF = PAD_K // 2
THIRD = HALF // 3
ORDERS = (("x", "yz"), ("y", "xz"), ("z", "xy"))


def total_kernel(dc_ref, loss_ref, dout_ref, lout_ref, part_ref, out_ref, r0, acc, r1, mid, r2,
                 s0, v0, s1, v1, s2, v2, s3, v3, s4, v4, s5, v5):
    me = lax.axis_index("data")
    core = lax.rem(me, 2)
    mate = me + 1 - 2 * core
    lines = [group_of(me, a) for a, _ in ORDERS]
    planes = [group_of(me, p) for _, p in ORDERS]
    devs = [mate]
    for _, others in lines:
        devs += [d for _, d in others]
    for n, (_, others) in enumerate(planes):
        axes = ORDERS[n][1]
        devs += [d for (_, d), offs in zip(others, [o for o in itertools.product(range(4), repeat=2) if any(o)]) if all(offs)]
    part_ref[:NUM_K, :] = dc_ref[...]
    part_ref[NUM_K:NUM_K + 8, :] = loss_ref[...]
    part_ref[NUM_K + 8:, :] = jnp.zeros((PAD_K - NUM_K - 8, 128), jnp.float32)
    enter(devs)()
    mine = pl.multiple_of(core * HALF, HALF)
    theirs = pl.multiple_of((1 - core) * HALF, HALF)
    pending = []

    def send(src, dst, ssem, rsem, dev):
        c = pltpu.make_async_remote_copy(src, dst, ssem, rsem, device_id=(dev,), device_id_type=MESH)
        c.start()
        pending.append(c)

    def arrived(dst, ssem, rsem, dev):
        pltpu.make_async_remote_copy(dst, dst, ssem, rsem, device_id=(dev,), device_id_type=MESH).wait_recv()

    for j in range(3):
        send(part_ref.at[pl.ds(theirs + j * THIRD, THIRD)], r0.at[j], s0.at[j], v0.at[j], mate)
    for j in range(3):
        arrived(r0.at[j], s0.at[j], v0.at[j], mate)
        acc[j] = part_ref[pl.ds(mine + j * THIRD, THIRD), :] + r0[j]
        own, others = lines[j]
        for k, (slot, dev) in enumerate(others):
            send(acc.at[j, pl.ds(pl.multiple_of(slot * 128, 128), 128)], r1.at[j, own], s1.at[j, k], v1.at[j, own], dev)
        r1[j, own] = acc[j, pl.ds(pl.multiple_of(own * 128, 128), 128), :]
    for j in range(3):
        own, others = lines[j]
        for k, (slot, dev) in enumerate(others):
            arrived(r1.at[j, slot], s1.at[j, k], v1.at[j, slot], dev)
        mid[j] = (r1[j, 0] + r1[j, 1]) + (r1[j, 2] + r1[j, 3])
        own, others = planes[j]
        for k, (slot, dev) in enumerate(others):
            send(mid.at[j, pl.ds(pl.multiple_of(slot * 8, 8), 8)], r2.at[j, own], s2.at[j, k], v2.at[j, own], dev)
        r2[j, own] = mid[j, pl.ds(pl.multiple_of(own * 8, 8), 8), :]
    for j in range(3):
        own_line = lines[j][0]
        own, others = planes[j]
        for k, (slot, dev) in enumerate(others):
            arrived(r2.at[j, slot], s2.at[j, k], v2.at[j, slot], dev)
        total = r2[j, 0]
        for q in range(1, 16):
            total = total + r2[j, q]
        spot = pl.ds(pl.multiple_of(mine + j * THIRD + own_line * 128 + own * 8, 8), 8)
        out_ref[spot, :] = total
        for k, (slot, dev) in enumerate(others):
            send(out_ref.at[spot], out_ref.at[spot], s3.at[j, k], v3.at[j, own], dev)
    for j in range(3):
        own_line, line = lines[j]
        own, others = planes[j]
        base = mine + j * THIRD + own_line * 128
        for k, (slot, dev) in enumerate(others):
            arrived(out_ref.at[pl.ds(pl.multiple_of(base + slot * 8, 8), 8)], s3.at[j, k], v3.at[j, slot], dev)
        spot = pl.ds(pl.multiple_of(base, 128), 128)
        for k, (slot, dev) in enumerate(line):
            send(out_ref.at[spot], out_ref.at[spot], s4.at[j, k], v4.at[j, own_line], dev)
        send(out_ref.at[spot], out_ref.at[spot], s5.at[j, 3], v5.at[j, own_line], mate)
    for j in range(3):
        own_line, line = lines[j]
        for k, (slot, dev) in enumerate(line):
            spot = pl.ds(pl.multiple_of(mine + j * THIRD + slot * 128, 128), 128)
            arrived(out_ref.at[spot], s4.at[j, k], v4.at[j, slot], dev)
            send(out_ref.at[spot], out_ref.at[spot], s5.at[j, k], v5.at[j, slot], mate)
    for j in range(3):
        for p in range(4):
            spot = pl.ds(pl.multiple_of(theirs + j * THIRD + p * 128, 128), 128)
            arrived(out_ref.at[spot], s5.at[j, 0], v5.at[j, p], mate)
    dout_ref[...] = out_ref[:NUM_K, :]
    lout_ref[...] = out_ref[NUM_K:NUM_K + 8, :]
    for c in pending:
        c.wait_send()


def run_total(part, loss):
    vmem = pl.BlockSpec(memory_space=pltpu.VMEM)
    dma = pltpu.SemaphoreType.DMA
    f32 = jnp.float32
    return pl.pallas_call(
        total_kernel,
        out_shape=(jax.ShapeDtypeStruct((NUM_K, 128), f32), jax.ShapeDtypeStruct((8, 128), f32)),
        in_specs=[vmem, vmem],
        out_specs=(vmem, vmem),
        scratch_shapes=[
            pltpu.VMEM((PAD_K, 128), f32),
            pltpu.VMEM((PAD_K, 128), f32),
            pltpu.VMEM((3, THIRD, 128), f32),
            pltpu.VMEM((3, THIRD, 128), f32),
            pltpu.VMEM((3, 4, 128, 128), f32),
            pltpu.VMEM((3, 128, 128), f32),
            pltpu.VMEM((3, 16, 8, 128), f32),
            dma((3,)), dma((3,)), dma((3, 3)), dma((3, 4)), dma((3, 15)), dma((3, 16)),
            dma((3, 15)), dma((3, 16)), dma((3, 3)), dma((3, 4)), dma((3, 4)), dma((3, 4)),
        ],
        name="total",
        compiler_params=pltpu.CompilerParams(collective_id=1, has_side_effects=True, vmem_limit_bytes=16 << 20),
    )(part, loss)


def finish_kernel(dc_ref, sum_ref, live_ref, out_ref, loss_ref, sem):
    copy = pltpu.make_async_copy(dc_ref, out_ref, sem)
    copy.start()
    total = jnp.sum(jnp.sum(sum_ref[...], axis=0, keepdims=True), axis=1, keepdims=True)
    loss_ref[...] = -total / (live_ref[0:1, 0:1] * 10.0)
    copy.wait()


def run_finish(total, loss_sum, live):
    vmem = pl.BlockSpec(memory_space=pltpu.VMEM)
    return pl.pallas_call(
        finish_kernel,
        out_shape=(jax.ShapeDtypeStruct((NUM_K, 128), jnp.float32), jax.ShapeDtypeStruct((1, 1), jnp.float32)),
        in_specs=[vmem] * 3,
        out_specs=(pl.BlockSpec(memory_space=pltpu.HBM), vmem),
        scratch_shapes=[pltpu.SemaphoreType.DMA],
        name="finish",
        compiler_params=pltpu.CompilerParams(vmem_limit_bytes=8 << 20),
    )(total, loss_sum, live)


def local_step(z_one, z_two, z_small, protos, live_mask):
    b, rows, live, z, c, mix, *t = run_codes(z_one, z_two, z_small, protos, live_mask[None, :])
    q_one, q_two, dz_one, dz_two, dz_small, part, loss = run_grads(z, c, b, rows, live, mix, t)
    total, loss_sum = run_total(part, loss)
    d_protos, loss_total = run_finish(total, loss_sum, live)
    return q_one.T, q_two.T, loss_total.reshape(()), dz_one, dz_two, dz_small, d_protos


def solution(mesh):
    row_spec = P("data", None)
    crop_spec = P(None, "data", None)
    return jax.shard_map(local_step, mesh=mesh,
                         in_specs=(row_spec, row_spec, crop_spec, P(None, None), P("data")),
                         out_specs=(row_spec, row_spec, P(), row_spec, row_spec, crop_spec, P(None, None)),
                         check_vma=False)
```
